32 devices in a mesh: member: 2 (over core), tp: 16 (over z, y, x).
Axes of the slice: x: 2, y: 2, z: 4, core: 2. Of those that a mesh axis runs over, the one named last changes fastest.
Arguments:
- stream_in: bfloat16 [512, 4096], P(('member', 'tp')), may hold values from -6 to 6
- kv_cache: bfloat16 [512, 512, 2048], P(('member', 'tp')), may hold values from -400 to 400
- lengths: int32 [128], replicated, may hold values from 1 to 512
- targets: int32 [128], replicated, may hold values from 0 to 65535
- norm_gains: float32 [3, 4096], replicated, may hold values from 0.1 to 1.9
- w_qkv: bfloat16 [4096, 6144], P(None, 'tp'), may hold values from -0.09375 to 0.09375
- w_out: bfloat16 [4096, 4096], P('tp'), may hold values from -0.09375 to 0.09375
- w_gate_up: bfloat16 [2, 4096, 14336], P(None, None, 'tp'), may hold values from -0.09375 to 0.09375
- w_down: bfloat16 [14336, 4096], P('tp'), may hold values from -0.046875 to 0.046875
- lm_head: bfloat16 [4096, 65536], P(None, 'tp'), may hold values from -300 to 300
- fast_in: float32 [4, 2, 4096], P('member'), may hold values from 0.1 to 1.9
- fast_hidden: float32 [4, 3, 14336], P('member', None, 'tp'), may hold values from 0.1 to 1.9
- fast_out: float32 [4, 4096], P('member'), may hold values from 0.1 to 1.9
Outputs:
- mean_logits: bfloat16 [128, 65536], P(None, 'tp')
- token_logprob: float32 [128], replicated
The draws below stay inside these ranges and needn't reach their ends.
Inputs may be any that keep to these rules, and one draw needn't show every extreme that they name: lengths is the same for all members.
All inputs are finite; a program needn't handle non-finite values.
Results may differ from the reference program's by a relative error of at most 0.02.
Values may be sent and summed in bfloat16 or wider, within the bound.
A program may use at most 192 MiB of HBM per device.

```python
import math
import jax
import jax.numpy as jnp
import numpy as np
from jax import lax

D = 4096
HEADS = 32
KV = 8
HD = 128
FF = 14336
VOCAB = 65536
B = 128
CACHE = 512
MEMBERS = 4


def draw_kv_cache(key, part):
    row_total = MEMBERS * B
    array_shape = (row_total, CACHE, 2 * KV * HD)
    key_main = jax.random.fold_in(key, 11)
    raw_draw = jnp.clip(jax.random.normal(key_main, array_shape, jnp.float32), -6.0, 6.0)
    return raw_draw.astype(jnp.bfloat16)


def draw_lm_head(key, part):
    array_shape = (D, VOCAB)
    key_main = jax.random.fold_in(key, 61)
    spread_scale = 3.0 / math.sqrt(D)
    result = jnp.clip(jax.random.normal(key_main, array_shape, jnp.float32) * spread_scale, -6.0 * spread_scale, 6.0 * spread_scale)
    return result.astype(jnp.bfloat16)


def with_ends(values, stream_key, low, largest):
    longest = values.shape.index(max(values.shape))
    spots = []
    for shift in (0, 1):
        where = [jax.random.randint(jax.random.fold_in(stream_key, axis), (), 0, length) for axis, length in enumerate(values.shape)]
        where[longest] = (where[longest] + shift) % values.shape[longest]
        spots.append(tuple(where))
    return values.at[spots[0]].set(low).at[spots[1]].set(largest)


def shard_levels(own_key, shape, shards, least, high):
    def one(axis_at, blocks):
        steps = jax.random.uniform(jax.random.fold_in(jax.random.fold_in(own_key, 6), axis_at), (blocks,), jnp.float32, least / len(shards), high / len(shards))
        return jnp.repeat(jnp.exp(steps), shape[axis_at] // blocks).reshape((-1,) + (1,) * (len(shape) - axis_at - 1))

    factor_of = one(*shards[0])
    for cut in shards[1:]:
        factor_of = factor_of * one(*cut)
    return factor_of


def rank_bounds(amount, skew):
    portions = [(1 << 20) // math.isqrt(grade ** skew) + 1 for grade in range(1, amount + 1)]
    deviation = 1 + sum(portions) // (1 << 30)
    return np.cumsum(np.array([max(1, weight // deviation) for weight in portions]))


def skewed_ids(stream_key, shape, number_of, slope):
    grid = rank_bounds(number_of, slope)
    lot = jax.random.randint(jax.random.fold_in(stream_key, 1), shape, 0, int(grid[number_of - 1]))
    grade = jnp.searchsorted(jnp.asarray(grid, jnp.int32), lot, side="right")
    return jax.random.permutation(jax.random.fold_in(stream_key, 2), number_of)[grade].astype(jnp.int32)


def noise(rng, shape, scale, most, cuts=(), held_as=jnp.bfloat16):
    values = scale * jax.random.normal(rng, shape, jnp.float32)
    if cuts:
        values = values * shard_levels(rng, shape, cuts, -0.22, 0.18)
    return jnp.clip(values, -most, most).astype(held_as)


def setup_inputs(seed: int = 0) -> dict:
    keys = jax.random.split(jax.random.key(seed), 14)
    return {
        "stream_in": noise(keys[0], (MEMBERS * B, D), 1.0, 6.0, ((0, 32),)),
        "kv_cache": draw_kv_cache(jax.random.fold_in(keys[13], 71), 0),
        "lengths": with_ends(jax.random.randint(keys[2], (B,), 1, CACHE + 1), jax.random.fold_in(keys[2], 1), 1, CACHE).astype(jnp.int32),
        "targets": with_ends(skewed_ids(keys[3], (B,), VOCAB, 2), jax.random.fold_in(keys[3], 3), 0, VOCAB - 1).astype(jnp.int32),
        "norm_gains": jnp.clip(1.0 + 0.18 * jax.random.normal(keys[4], (3, D), jnp.float32), 0.1, 1.9),
        "w_qkv": noise(keys[5], (D, (HEADS + 2 * KV) * HD), D ** -0.5, 0.09375, ((1, 16),)),
        "w_out": noise(keys[6], (HEADS * HD, D), (HEADS * HD) ** -0.5, 0.09375, ((0, 16),)),
        "w_gate_up": noise(keys[7], (2, D, FF), D ** -0.5, 0.09375, ((2, 16),)),
        "w_down": noise(keys[8], (FF, D), FF ** -0.5, 0.046875, ((0, 16),)),
        "lm_head": draw_lm_head(jax.random.fold_in(keys[13], 71), 0),
        "fast_in": jnp.clip(1.0 + 0.18 * jax.random.normal(keys[10], (MEMBERS, 2, D), jnp.float32), 0.1, 1.9),
        "fast_hidden": jnp.clip(1.0 + 0.18 * jax.random.normal(keys[11], (MEMBERS, 3, FF), jnp.float32), 0.1, 1.9),
        "fast_out": jnp.clip(1.0 + 0.18 * jax.random.normal(keys[12], (MEMBERS, D), jnp.float32), 0.1, 1.9),
    }


ROPE_BASE = 500000.0

def rms_norm(values_in, gain):
    return values_in * lax.rsqrt(lax.optimization_barrier(jnp.mean(values_in * values_in, axis=-1, keepdims=True)) + 1e-05) * gain

def rotate(values_in, positions):
    half_dim = values_in.shape[-1] // 2
    frequency = ROPE_BASE ** (-jnp.arange(half_dim, dtype=jnp.float32) * 2.0 / values_in.shape[-1])
    angles = positions.astype(jnp.float32)[:, None, None] * frequency[None, None, :]
    lower_half = values_in[..., :half_dim]
    upper_half = values_in[..., half_dim:]
    return jnp.concatenate([lower_half * jnp.cos(angles) - upper_half * jnp.sin(angles), upper_half * jnp.cos(angles) + lower_half * jnp.sin(angles)], axis=-1)

def attend(projected, cache_rows, positions):
    row_count = projected.shape[0]
    head_cols = HEADS * HD
    kv_cols = KV * HD
    queries = rotate(projected[:, :head_cols].astype(jnp.float32).reshape(row_count, HEADS, HD), positions).astype(jnp.bfloat16)
    new_key = rotate(projected[:, head_cols:head_cols + kv_cols].astype(jnp.float32).reshape(row_count, KV, HD), positions).astype(jnp.bfloat16)
    new_value = projected[:, head_cols + kv_cols:].reshape(row_count, KV, HD)
    cache_keys = cache_rows[:, :, :kv_cols].reshape(row_count, CACHE, KV, HD)
    cache_values = cache_rows[:, :, kv_cols:].reshape(row_count, CACHE, KV, HD)
    grouped = queries.reshape(row_count, KV, HEADS // KV, HD).astype(jnp.float32)
    inv_root = HD ** (-0.5)
    cached = jnp.einsum('rkgd,rckd->rkgc', grouped, cache_keys.astype(jnp.float32)) * inv_root
    fresh = jnp.einsum('rkgd,rkd->rkg', grouped, new_key.astype(jnp.float32)) * inv_root
    in_cache = jnp.arange(CACHE)[None, :] < positions[:, None]
    cached = jnp.where(in_cache[:, None, None, :], cached, -1e+30)
    peak = jnp.maximum(lax.optimization_barrier(jnp.max(cached, axis=-1)), fresh)
    weights = jnp.exp(cached - peak[..., None])
    fresh_w = jnp.exp(fresh - peak)
    total_sum = lax.optimization_barrier(jnp.sum(weights, axis=-1)) + fresh_w
    probs = (weights / total_sum[..., None]).astype(jnp.bfloat16)
    fresh_p = (fresh_w / total_sum).astype(jnp.bfloat16)
    result = jnp.einsum('rkgc,rckd->rkgd', probs.astype(jnp.float32), cache_values.astype(jnp.float32))
    result = result + fresh_p.astype(jnp.float32)[..., None] * new_value.astype(jnp.float32)[:, :, None, :]
    return result.reshape(row_count, HEADS * HD).astype(jnp.bfloat16)

def reference(stream_in, kv_cache, lengths, targets, norm_gains, w_qkv, w_out, w_gate_up, w_down, lm_head, fast_in, fast_hidden, fast_out):
    row_count = stream_in.shape[0]
    positions = jnp.tile(lengths, MEMBERS).astype(jnp.int32)
    attn_in = rms_norm(stream_in.astype(jnp.float32), norm_gains[0]).astype(jnp.bfloat16)
    projected = jnp.dot(attn_in, w_qkv, preferred_element_type=jnp.float32).astype(jnp.bfloat16)
    blocks = lax.map(lambda block_item: attend(block_item[0], block_item[1], block_item[2]), (projected.reshape(row_count // 8, 8, -1), kv_cache.reshape(row_count // 8, 8, CACHE, 2 * KV * HD), positions.reshape(row_count // 8, 8)))
    attended = blocks.reshape(row_count, HEADS * HD)
    middle = (stream_in.astype(jnp.float32) + jnp.dot(attended, w_out, preferred_element_type=jnp.float32)).astype(jnp.bfloat16)
    ffn_in = rms_norm(middle.astype(jnp.float32), norm_gains[1]).astype(jnp.bfloat16)
    grouped = ffn_in.astype(jnp.float32).reshape(MEMBERS, B, D)
    gate_in = (grouped * fast_in[:, 0][:, None, :]).astype(jnp.bfloat16).reshape(row_count, D)
    up_in = (grouped * fast_in[:, 1][:, None, :]).astype(jnp.bfloat16).reshape(row_count, D)
    gate_act = jnp.dot(gate_in, w_gate_up[0], preferred_element_type=jnp.float32).reshape(MEMBERS, B, FF) * fast_hidden[:, 0][:, None, :]
    up_act = jnp.dot(up_in, w_gate_up[1], preferred_element_type=jnp.float32).reshape(MEMBERS, B, FF) * fast_hidden[:, 1][:, None, :]
    hidden = (jax.nn.silu(gate_act) * up_act * fast_hidden[:, 2][:, None, :]).astype(jnp.bfloat16).reshape(row_count, FF)
    down_sum = jnp.dot(hidden, w_down, preferred_element_type=jnp.float32).reshape(MEMBERS, B, D) * fast_out[:, None, :]
    layer_out = (middle.astype(jnp.float32).reshape(MEMBERS, B, D) + down_sum).astype(jnp.bfloat16).reshape(row_count, D)
    final_in = rms_norm(layer_out.astype(jnp.float32), norm_gains[2]).astype(jnp.bfloat16)
    logits = jnp.dot(final_in, lm_head, preferred_element_type=jnp.float32)
    mean_logit = lax.optimization_barrier(jnp.sum(logits.reshape(MEMBERS, B, VOCAB), axis=0)) / MEMBERS
    peak = lax.optimization_barrier(jnp.max(mean_logit, axis=-1))
    log_total = peak + jnp.log(lax.optimization_barrier(jnp.sum(jnp.exp(mean_logit - peak[:, None]), axis=-1)))
    target_logit = lax.optimization_barrier(jnp.sum(jnp.where(jnp.arange(VOCAB)[None, :] == targets[:, None], mean_logit, 0.0), axis=-1))
    return (mean_logit.astype(jnp.bfloat16), target_logit - log_total)
```

```python
import functools

import jax
import jax.numpy as jnp
from jax import lax
from jax.experimental import pallas as pl
from jax.experimental.pallas import tpu as pltpu
from jax.sharding import PartitionSpec as P

HEADS = 32
KV = 8
HD = 128
CACHE = 512


ROPE_BASE = 500000.0


def rms_norm(values_in, gain):
    return (
        values_in
        * lax.rsqrt(jnp.mean(values_in * values_in, axis=-1, keepdims=True) + 1e-05)
        * gain
    )


def rotate(values_in, positions):
    half_dim = values_in.shape[-1] // 2
    frequency = ROPE_BASE ** (-jnp.arange(half_dim, dtype=jnp.float32) * 2.0 / values_in.shape[-1])
    angles = positions.astype(jnp.float32)[:, None, None] * frequency[None, None, :]
    lower_half = values_in[..., :half_dim]
    upper_half = values_in[..., half_dim:]
    return jnp.concatenate(
        [
            lower_half * jnp.cos(angles) - upper_half * jnp.sin(angles),
            upper_half * jnp.cos(angles) + lower_half * jnp.sin(angles),
        ],
        axis=-1,
    )


def attend(projected, cache_rows, positions):
    row_count = projected.shape[0]
    head_cols = HEADS * HD
    kv_cols = KV * HD
    queries = rotate(
        projected[:, :head_cols].astype(jnp.float32).reshape(row_count, HEADS, HD), positions
    ).astype(jnp.bfloat16)
    new_key = rotate(
        projected[:, head_cols : head_cols + kv_cols]
        .astype(jnp.float32)
        .reshape(row_count, KV, HD),
        positions,
    ).astype(jnp.bfloat16)
    new_value = projected[:, head_cols + kv_cols :].reshape(row_count, KV, HD)
    cache_keys = cache_rows[:, :, :kv_cols].reshape(row_count, CACHE, KV, HD)
    cache_values = cache_rows[:, :, kv_cols:].reshape(row_count, CACHE, KV, HD)
    grouped = queries.reshape(row_count, KV, HEADS // KV, HD)
    inv_root = HD ** (-0.5)
    cached = (
        jnp.einsum("rkgd,rckd->rkgc", grouped, cache_keys, preferred_element_type=jnp.float32)
        * inv_root
    )
    fresh = (
        jnp.einsum("rkgd,rkd->rkg", grouped, new_key, preferred_element_type=jnp.float32) * inv_root
    )
    in_cache = jnp.arange(CACHE)[None, :] < positions[:, None]
    cached = jnp.where(in_cache[:, None, None, :], cached, -1e30)
    peak = jnp.maximum(jnp.max(cached, axis=-1), fresh)
    weights = jnp.exp(cached - peak[..., None])
    fresh_w = jnp.exp(fresh - peak)
    total_sum = jnp.sum(weights, axis=-1) + fresh_w
    probs = (weights / total_sum[..., None]).astype(jnp.bfloat16)
    fresh_p = (fresh_w / total_sum).astype(jnp.bfloat16)
    result = jnp.einsum("rkgc,rckd->rkgd", probs, cache_values, preferred_element_type=jnp.float32)
    result = (
        result
        + fresh_p.astype(jnp.float32)[..., None] * new_value.astype(jnp.float32)[:, :, None, :]
    )
    return result.reshape(row_count, HEADS * HD).astype(jnp.bfloat16)


def plain_body(
    stream_in,
    kv_cache,
    lengths,
    targets,
    norm_gains,
    w_qkv,
    w_out,
    w_gate_up,
    w_down,
    lm_head,
    fast_in,
    fast_hidden,
    fast_out,
):
    tp_count = lax.axis_size("tp")
    tp_rank = lax.axis_index("tp")
    mem_dev = fast_in.shape[0]
    batch_rows = lengths.shape[0]
    own_rows = stream_in.shape[0]
    all_rows = own_rows * tp_count
    width = stream_in.shape[1]
    first_row = tp_rank * own_rows
    positions = lax.dynamic_slice_in_dim(lengths, first_row % batch_rows, own_rows, 0)
    own_member = first_row // batch_rows
    own_scale = lax.dynamic_index_in_dim(fast_out, own_member, 0, keepdims=True)
    own_normed = rms_norm(stream_in.astype(jnp.float32), norm_gains[0]).astype(jnp.bfloat16)
    attn_in = lax.all_gather(own_normed, "tp", axis=0, tiled=True)
    projected = jnp.dot(attn_in, w_qkv, preferred_element_type=jnp.float32).astype(jnp.bfloat16)
    row_major = lax.all_to_all(projected, "tp", split_axis=0, concat_axis=1, tiled=True)
    attended = attend(row_major, kv_cache, positions)
    head_major = lax.all_to_all(attended, "tp", split_axis=1, concat_axis=0, tiled=True)
    picked = head_major
    attn_sum = lax.psum_scatter(
        jnp.dot(picked, w_out, preferred_element_type=jnp.float32),
        "tp",
        scatter_dimension=0,
        tiled=True,
    )
    middle = (stream_in.astype(jnp.float32) + attn_sum).astype(jnp.bfloat16)
    own_ffn = rms_norm(middle.astype(jnp.float32), norm_gains[1]).astype(jnp.bfloat16)
    ffn_in = lax.all_gather(own_ffn, "tp", axis=0, tiled=True)
    grouped = ffn_in.astype(jnp.float32).reshape(mem_dev, batch_rows, width)
    gate_in = (grouped * fast_in[:, 0][:, None, :]).astype(jnp.bfloat16).reshape(all_rows, width)
    up_in = (grouped * fast_in[:, 1][:, None, :]).astype(jnp.bfloat16).reshape(all_rows, width)
    hidden_cols = w_gate_up.shape[2]
    gate_act = (
        jnp.dot(gate_in, w_gate_up[0], preferred_element_type=jnp.float32).reshape(
            mem_dev, batch_rows, hidden_cols
        )
        * fast_hidden[:, 0][:, None, :]
    )
    up_act = (
        jnp.dot(up_in, w_gate_up[1], preferred_element_type=jnp.float32).reshape(
            mem_dev, batch_rows, hidden_cols
        )
        * fast_hidden[:, 1][:, None, :]
    )
    hidden = (
        (jax.nn.silu(gate_act) * up_act * fast_hidden[:, 2][:, None, :])
        .astype(jnp.bfloat16)
        .reshape(all_rows, hidden_cols)
    )
    picked = hidden
    down_sum = lax.psum_scatter(
        jnp.dot(picked, w_down, preferred_element_type=jnp.float32),
        "tp",
        scatter_dimension=0,
        tiled=True,
    )
    layer_out = (middle.astype(jnp.float32) + down_sum * own_scale).astype(jnp.bfloat16)
    own_final = rms_norm(layer_out.astype(jnp.float32), norm_gains[2]).astype(jnp.bfloat16)
    final_in = lax.all_gather(own_final, "tp", axis=0, tiled=True)
    logits = jnp.dot(final_in, lm_head, preferred_element_type=jnp.float32)
    vocab_cols = lm_head.shape[1]
    member_total = jnp.sum(logits.reshape(mem_dev, batch_rows, vocab_cols), axis=0)
    member_count = mem_dev * lax.axis_size("member")
    mean_logit = (
        lax.psum(member_total.astype(jnp.bfloat16), "member").astype(jnp.float32) / member_count
    )
    column_ids = tp_rank * vocab_cols + jnp.arange(vocab_cols)
    target_part = jnp.sum(
        jnp.where(column_ids[None, :] == targets[:, None], mean_logit, 0.0), axis=-1
    )
    local_peak = jnp.max(mean_logit, axis=-1)
    peak = lax.pmax(local_peak, "tp")
    exp_total, target_logit = lax.psum(
        (jnp.sum(jnp.exp(mean_logit - peak[:, None]), axis=-1), target_part), "tp"
    )
    token_logprob = target_logit - (peak + jnp.log(exp_total))
    return (mean_logit.astype(jnp.bfloat16), token_logprob)


BF16 = jnp.bfloat16
F32 = jnp.float32
DMA = pltpu.SemaphoreType.DMA
QUAD = 4


def norm_rows(values_in, gain):
    return (
        values_in
        * lax.rsqrt(jnp.mean(values_in * values_in, axis=-1, keepdims=True) + 1e-05)
        * gain
    )


class Place:
    def __init__(self, lines):
        self.tp = lax.axis_index("tp")
        self.member = lax.axis_index("member")
        self.lines = lines
        self.quad = lax.rem(self.tp, QUAD)
        self.line = self.tp // QUAD
        self.quad_x = self.quad + 1 - 2 * lax.rem(self.quad, 2)
        self.quad_y = lax.rem(self.quad + 2, QUAD)
        self.quad_d = self.quad_x + self.quad_y - self.quad
        self.to_x = {"tp": self.line * QUAD + self.quad_x}
        self.to_y = {"tp": self.line * QUAD + self.quad_y}

    def line_at(self, step):
        return lax.rem(self.line + step + self.lines, self.lines)

    def to_line(self, step):
        return {"tp": self.line_at(step) * QUAD + self.quad}


def remote(src, dst, send_sem, recv_sem, device):
    copy = pltpu.make_async_remote_copy(
        src_ref=src,
        dst_ref=dst,
        send_sem=send_sem,
        recv_sem=recv_sem,
        device_id=device,
        device_id_type=pl.DeviceIdType.MESH,
    )
    copy.start()
    return copy


def greet(devices):
    barrier = pltpu.get_barrier_semaphore()
    for device in devices:
        pl.semaphore_signal(
            barrier, inc=1, device_id=device, device_id_type=pl.DeviceIdType.MESH
        )
    pl.semaphore_wait(barrier, len(devices))


def gather_rows(place, own, out, sems, line_steps, block_of):
    local_sem, sends, recvs = sems
    rows, cols = own.shape
    half = cols // 2

    def rows_of(step, quad):
        return pl.ds(pl.multiple_of(block_of(step, quad) * rows, rows), rows)

    mine = out.at[rows_of(0, place.quad)]
    local = pltpu.make_async_copy(own, mine, local_sem)
    local.start()
    line_copies = []
    for k, step in enumerate(line_steps):
        if k:
            line_copies.append(
                remote(own, mine, sends.at[0, k], recvs.at[0, k], place.to_line(step))
            )
        else:
            line_copies.append(None)
    by_x, by_y, over_x, over_y = [], [], [], []

    def spread(k):
        block = own if k == 0 else out.at[rows_of(-line_steps[k], place.quad)]
        into = out.at[rows_of(-line_steps[k], place.quad)]
        by_x.append(remote(block, into, sends.at[1, k], recvs.at[1, k], place.to_x))
        by_y.append(remote(block, into, sends.at[2, k], recvs.at[2, k], place.to_y))

    def relay(k):
        by_x[k].wait_recv()
        from_x = out.at[rows_of(-line_steps[k], place.quad_x), pl.ds(0, half)]
        over_y.append(remote(from_x, from_x, sends.at[3, k], recvs.at[3, k], place.to_y))
        by_y[k].wait_recv()
        from_y = out.at[rows_of(-line_steps[k], place.quad_y), pl.ds(half, half)]
        over_x.append(remote(from_y, from_y, sends.at[4, k], recvs.at[4, k], place.to_x))

    spread(0)
    for k in range(1, len(line_steps)):
        line_copies[k].wait_recv()
        spread(k)
        relay(k - 1)
    relay(len(line_steps) - 1)
    for k in range(len(line_steps)):
        over_y[k].wait_recv()
        over_x[k].wait_recv()
    local.wait()
    for copies in (line_copies, by_x, by_y, over_x, over_y):
        for copy in copies:
            if copy is not None:
                copy.wait_send()


def sum_rows(place, part, sems, bufs):
    sends, recvs = sems
    got_dx, got_dy, put_x, put_y, got_x, got_y, put_z, got_z = bufs
    rows = got_x.shape[1]
    half = got_dx.shape[2]
    low, high = pl.ds(0, half), pl.ds(half, half)
    steps = list(range(1, place.lines)) + [0]

    def rows_of(step, quad):
        index = place.line_at(step) * QUAD + quad
        return pl.ds(pl.multiple_of(index * rows, rows), rows)

    d_x, d_y, x_high, y_low, x_low, y_high, z_copies = {}, {}, {}, {}, {}, {}, {}
    for k in steps:
        diag = rows_of(k, place.quad_d)
        d_x[k] = remote(part.at[diag, high], got_dx.at[k], sends.at[0, k], recvs.at[0, k], place.to_x)
        d_y[k] = remote(part.at[diag, low], got_dy.at[k], sends.at[1, k], recvs.at[1, k], place.to_y)
    for k in steps:
        x_high[k] = remote(
            part.at[rows_of(k, place.quad_x), high], got_x.at[k, :, high],
            sends.at[2, k], recvs.at[2, k], place.to_x,
        )
        y_low[k] = remote(
            part.at[rows_of(k, place.quad_y), low], got_y.at[k, :, low],
            sends.at[3, k], recvs.at[3, k], place.to_y,
        )
        d_y[k].wait_recv()
        put_x[k] = (
            part[rows_of(k, place.quad_x), low].astype(F32) + got_dy[k].astype(F32)
        ).astype(BF16)
        x_low[k] = remote(
            put_x.at[k], got_x.at[k, :, low], sends.at[4, k], recvs.at[4, k], place.to_x
        )
        d_x[k].wait_recv()
        put_y[k] = (
            part[rows_of(k, place.quad_y), high].astype(F32) + got_dx[k].astype(F32)
        ).astype(BF16)
        y_high[k] = remote(
            put_y.at[k], got_y.at[k, :, high], sends.at[5, k], recvs.at[5, k], place.to_y
        )
    total = None
    for k in steps:
        for copies in (x_high, y_low, x_low, y_high):
            copies[k].wait_recv()
        quad_sum = (
            part[rows_of(k, place.quad), :].astype(F32)
            + got_x[k].astype(F32)
            + got_y[k].astype(F32)
        )
        if k:
            put_z[k] = quad_sum.astype(BF16)
            z_copies[k] = remote(
                put_z.at[k], got_z.at[k], sends.at[6, k], recvs.at[6, k], place.to_line(k)
            )
        else:
            total = quad_sum
    for k in steps[:-1]:
        z_copies[k].wait_recv()
        total = total + got_z[k].astype(F32)
    for copies in (d_x, d_y, x_high, y_low, x_low, y_high, z_copies):
        for copy in copies.values():
            copy.wait_send()
    return total


def near(place):
    return [place.to_x, place.to_y] + [place.to_line(k) for k in range(1, place.lines)]


def gather_kernel(lines, stream, gain, out, own, local_sem, sends, recvs):
    place = Place(lines)
    own[...] = norm_rows(stream[...].astype(F32), gain[...]).astype(BF16)
    greet(near(place))
    gather_rows(
        place, own, out, (local_sem, sends, recvs), list(range(lines)),
        lambda step, quad: place.line_at(step) * QUAD + quad,
    )


def middle_kernel(
    lines, part, stream, gain, middle, out, own, local_sem, sends, recvs, sum_sends, sum_recvs, *bufs
):
    place = Place(lines)
    greet(near(place))
    total = sum_rows(place, part, (sum_sends, sum_recvs), bufs)
    middle[...] = (stream[...].astype(F32) + total).astype(BF16)
    own[...] = norm_rows(middle[...].astype(F32), gain[...]).astype(BF16)
    gather_rows(
        place, own, out, (local_sem, sends, recvs), list(range(lines)),
        lambda step, quad: place.line_at(step) * QUAD + quad,
    )


def final_kernel(
    lines, part, middle, scale, gain, out,
    own, away, from_core, pair, from_pair, mean,
    local_sem, sends, recvs, side_sends, side_recvs, sum_sends, sum_recvs, *bufs
):
    place = Place(lines)
    other = {"member": 1 - place.member}
    greet(near(place) + [other])
    total = sum_rows(place, part, (sum_sends, sum_recvs), bufs)
    layer_out = (middle[...].astype(F32) + total * scale[...]).astype(BF16)
    normed = norm_rows(layer_out.astype(F32), gain[...]).astype(BF16)
    half = mean.shape[1]
    first = place.member == 0
    low, high = normed[:, :half], normed[:, half:]
    own[...] = jnp.where(first, low.astype(F32), high.astype(F32))
    away[...] = jnp.where(first, high.astype(F32), low.astype(F32)).astype(BF16)
    core = remote(away, from_core, side_sends.at[0], side_recvs.at[0], other)
    core.wait_recv()
    own[...] = own[...] + from_core[...].astype(F32)
    pair[...] = own[...]
    twin = remote(
        pair, from_pair, side_sends.at[1], side_recvs.at[1], place.to_line(lines // 2)
    )
    twin.wait_recv()
    mean[...] = ((own[...] + from_pair[...]) * 0.25).astype(BF16)
    turn = 1 - 2 * lax.rem(place.line, 2)

    class Pairwise:
        pass

    near_line = Pairwise()
    near_line.quad, near_line.quad_x, near_line.quad_y = place.quad, place.quad_x, place.quad_y
    near_line.to_x, near_line.to_y = place.to_x, place.to_y
    near_line.to_line = lambda step: {"tp": (place.line + turn) * QUAD + place.quad}
    mine = out.at[place.member]
    gather_rows(
        near_line, mean, mine, (local_sem, sends, recvs), [0, 1],
        lambda step, quad: lax.rem(place.line + abs(step), 2) * QUAD + quad,
    )
    share = remote(mine, mine, side_sends.at[2], side_recvs.at[2], other)
    share.wait_recv()
    for copy in (core, twin, share):
        copy.wait_send()


VMEM = pl.BlockSpec(memory_space=pltpu.VMEM)
VMEM_BYTES = 60 * 1024 * 1024


def call_linked(kernel, number, out_shape, scratch, args):
    return pl.pallas_call(
        kernel,
        out_shape=out_shape,
        in_specs=[VMEM] * len(args),
        out_specs=jax.tree.map(lambda _: VMEM, out_shape),
        scratch_shapes=scratch,
        compiler_params=pltpu.CompilerParams(
            collective_id=number, has_side_effects=True, vmem_limit_bytes=VMEM_BYTES
        ),
    )(*args)


def gather_scratch(lines):
    return [DMA, DMA((5, lines)), DMA((5, lines))]


def sum_scratch(lines, rows, cols):
    small = pltpu.VMEM((lines, rows, cols // 2), BF16)
    large = pltpu.VMEM((lines, rows, cols), BF16)
    return [DMA((7, lines)), DMA((7, lines)), small, small, small, small, large, large, large, large]


def attend_kernel(positions, query, fresh_key, fresh_value, cache, out):
    row = pl.program_id(0)
    heads, head_size = query.shape[1], query.shape[2]
    kv_cols = cache.shape[2] // 2
    key_heads = kv_cols // head_size
    group = heads // key_heads
    count = cache.shape[1]
    query_row = query[0].astype(F32)
    inv_root = head_size ** (-0.5)
    wide = jnp.concatenate([query_row] * key_heads, axis=1)
    owner = lax.broadcasted_iota(jnp.int32, wide.shape, 0) // group
    column = lax.broadcasted_iota(jnp.int32, wide.shape, 1) // head_size
    wide = jnp.where(owner == column, wide, 0.0).astype(BF16)
    scores = (
        lax.dot_general(
            wide, cache[0, :, :kv_cols], (((1,), (1,)), ((), ())), preferred_element_type=F32
        )
        * inv_root
    )
    spot = lax.broadcasted_iota(jnp.int32, scores.shape, 1)
    scores = jnp.where(spot < positions[row], scores, -1e30)
    fresh = jnp.sum(query_row * fresh_key[0].astype(F32), axis=-1, keepdims=True) * inv_root
    peak = jnp.maximum(jnp.max(scores, axis=-1, keepdims=True), fresh)
    weights = jnp.exp(scores - peak)
    fresh_w = jnp.exp(fresh - peak)
    total_sum = jnp.sum(weights, axis=-1, keepdims=True) + fresh_w
    probs = (weights / total_sum).astype(BF16)
    fresh_p = (fresh_w / total_sum).astype(BF16).astype(F32)
    full = jnp.dot(probs, cache[0, :, kv_cols:], preferred_element_type=F32)
    full = jnp.where(owner == column, full, 0.0)
    result = full[:, :head_size]
    for k in range(1, key_heads):
        result = result + full[:, k * head_size : (k + 1) * head_size]
    out[0] = (result + fresh_p * fresh_value[0].astype(F32)).astype(BF16)


def attend_rows(projected, cache_rows, positions):
    rows = projected.shape[0]
    head_cols, kv_cols = HEADS * HD, KV * HD
    group = HEADS // KV
    queries = rotate(
        projected[:, :head_cols].astype(F32).reshape(rows, HEADS, HD), positions
    ).astype(BF16)
    new_key = rotate(
        projected[:, head_cols : head_cols + kv_cols].astype(F32).reshape(rows, KV, HD), positions
    ).astype(BF16)
    new_value = projected[:, head_cols + kv_cols :].reshape(rows, KV, HD)
    new_key = jnp.repeat(new_key, group, axis=1)
    new_value = jnp.repeat(new_value, group, axis=1)
    per_row = pl.BlockSpec((1, HEADS, HD), lambda r, p: (r, 0, 0))
    cache_spec = pl.BlockSpec((1,) + cache_rows.shape[1:], lambda r, p: (r, 0, 0))
    result = pl.pallas_call(
        attend_kernel,
        grid_spec=pltpu.PrefetchScalarGridSpec(
            num_scalar_prefetch=1,
            grid=(rows,),
            in_specs=[per_row, per_row, per_row, cache_spec],
            out_specs=per_row,
        ),
        out_shape=jax.ShapeDtypeStruct((rows, HEADS, HD), BF16),
        compiler_params=pltpu.CompilerParams(vmem_limit_bytes=32 * 1024 * 1024),
    )(positions, queries, new_key, new_value, cache_rows)
    return result.reshape(rows, head_cols)


def score_kernel(place, rows_in, targets, weights, logits, stats, peak, total, found):
    step = pl.program_id(0)
    steps = pl.num_programs(0)
    depth = rows_in.shape[2]
    tile = jnp.dot(rows_in[0], weights[:depth, :], preferred_element_type=F32) + jnp.dot(
        rows_in[1], weights[depth:, :], preferred_element_type=F32
    )
    logits[...] = tile.astype(BF16)

    @pl.when(step == 0)
    def _():
        peak[...] = jnp.full_like(peak, -jnp.inf)
        total[...] = jnp.zeros_like(total)
        found[...] = jnp.zeros_like(found)

    old = peak[...]
    new = jnp.maximum(old, jnp.max(tile, axis=-1, keepdims=True))
    total[...] = total[...] * jnp.exp(old - new) + jnp.sum(
        jnp.exp(tile - new), axis=-1, keepdims=True
    )
    peak[...] = new
    column = (
        place[0] * tile.shape[1] * steps
        + step * tile.shape[1]
        + lax.broadcasted_iota(jnp.int32, tile.shape, 1)
    )
    found[...] += jnp.sum(jnp.where(column == targets[...], tile, 0.0), axis=-1, keepdims=True)

    @pl.when(step == steps - 1)
    def _():
        lane = lax.broadcasted_iota(jnp.int32, stats.shape, 1)
        stats[...] = jnp.where(
            lane == 0, peak[...], jnp.where(lane == 1, total[...], found[...])
        )


def score(rows_in, targets, lm_head, tile=256):
    _, batch_rows, depth = rows_in.shape
    vocab_cols = lm_head.shape[1]
    cols = vocab_cols // 2
    member = lax.axis_index("member")
    place = (lax.axis_index("tp") * 2 + member)[None].astype(jnp.int32)
    steps = cols // tile
    return pl.pallas_call(
        score_kernel,
        grid_spec=pltpu.PrefetchScalarGridSpec(
            num_scalar_prefetch=1,
            grid=(steps,),
            in_specs=[
                pl.BlockSpec(rows_in.shape, lambda s, p: (0, 0, 0)),
                pl.BlockSpec((batch_rows, 1), lambda s, p: (0, 0)),
                pl.BlockSpec((2 * depth, tile), lambda s, p: (0, lax.rem(p[0], 2) * steps + s)),
            ],
            out_specs=[
                pl.BlockSpec((batch_rows, tile), lambda s, p: (0, s)),
                pl.BlockSpec((batch_rows, 128), lambda s, p: (0, 0)),
            ],
            scratch_shapes=[pltpu.VMEM((batch_rows, 1), F32)] * 3,
        ),
        out_shape=[
            jax.ShapeDtypeStruct((batch_rows, cols), BF16),
            jax.ShapeDtypeStruct((batch_rows, 128), F32),
        ],
        compiler_params=pltpu.CompilerParams(vmem_limit_bytes=32 * 1024 * 1024),
    )(place, rows_in, targets[:, None], lm_head)


def close_kernel(tp_count, logits, stats, out, logprob, table, side_sem, sends, recvs):
    tp = lax.axis_index("tp")
    member = lax.axis_index("member")
    cols = logits.shape[1]
    others = []
    for other in range(2):
        for step in range(tp_count):
            if other or step:
                core = member if other == 0 else 1 - member
                others.append({"member": core, "tp": lax.rem(tp + step, tp_count)})
    greet(others)
    mine = out.at[:, pl.ds(pl.multiple_of(member * cols, cols), cols)]
    share = remote(logits, mine, sends.at[0], recvs.at[0], {"member": 1 - member})
    local = pltpu.make_async_copy(logits, mine, side_sem)
    local.start()
    copies = []
    for slot, device in enumerate(others):
        copies.append(
            remote(stats, table.at[slot + 1], sends.at[slot + 1], recvs.at[slot + 1], device)
        )
    table[0] = stats[...]
    for copy in copies:
        copy.wait_recv()
    peak = jnp.max(table[:, 0, :], axis=0, keepdims=True)
    total = jnp.sum(table[:, 1, :] * jnp.exp(table[:, 0, :] - peak), axis=0, keepdims=True)
    found = jnp.sum(table[:, 2, :], axis=0, keepdims=True)
    logprob[...] = found - (peak + jnp.log(total))
    share.wait_recv()
    local.wait()
    share.wait_send()
    for copy in copies:
        copy.wait_send()


def linked_body(
    stream_in,
    kv_cache,
    lengths,
    targets,
    norm_gains,
    w_qkv,
    w_out,
    w_gate_up,
    w_down,
    lm_head,
    fast_in,
    fast_hidden,
    fast_out,
):
    tp_count = lax.axis_size("tp")
    tp_rank = lax.axis_index("tp")
    lines = tp_count // QUAD
    mem_dev = fast_in.shape[0]
    batch_rows = lengths.shape[0]
    own_rows, width = stream_in.shape
    all_rows = own_rows * tp_count
    first_row = tp_rank * own_rows
    positions = lax.dynamic_slice_in_dim(lengths, first_row % batch_rows, own_rows, 0)
    own_member = first_row // batch_rows
    own_scale = lax.dynamic_index_in_dim(fast_out, own_member, 0, keepdims=True)
    own_shape = jax.ShapeDtypeStruct((own_rows, width), BF16)
    all_shape = jax.ShapeDtypeStruct((all_rows, width), BF16)
    own_buf = pltpu.VMEM((own_rows, width), BF16)

    attn_in = call_linked(
        functools.partial(gather_kernel, lines), 1, all_shape,
        [own_buf] + gather_scratch(lines), (stream_in, norm_gains[0:1]),
    )
    projected = jnp.dot(attn_in, w_qkv, preferred_element_type=F32).astype(BF16)
    row_major = lax.all_to_all(projected, "tp", split_axis=0, concat_axis=1, tiled=True)
    attended = attend_rows(row_major, kv_cache, positions)
    head_major = lax.all_to_all(attended, "tp", split_axis=1, concat_axis=0, tiled=True)
    attn_part = jnp.dot(head_major, w_out, preferred_element_type=F32).astype(BF16)
    middle, ffn_in = call_linked(
        functools.partial(middle_kernel, lines), 2, [own_shape, all_shape],
        [own_buf] + gather_scratch(lines) + sum_scratch(lines, own_rows, width),
        (attn_part, stream_in, norm_gains[1:2]),
    )
    grouped = ffn_in.astype(F32).reshape(mem_dev, batch_rows, width)
    gate_in = (grouped * fast_in[:, 0][:, None, :]).astype(BF16).reshape(all_rows, width)
    up_in = (grouped * fast_in[:, 1][:, None, :]).astype(BF16).reshape(all_rows, width)
    hidden_cols = w_gate_up.shape[2]
    gate_act = (
        jnp.dot(gate_in, w_gate_up[0], preferred_element_type=F32).reshape(
            mem_dev, batch_rows, hidden_cols
        )
        * fast_hidden[:, 0][:, None, :]
    )
    up_act = (
        jnp.dot(up_in, w_gate_up[1], preferred_element_type=F32).reshape(
            mem_dev, batch_rows, hidden_cols
        )
        * fast_hidden[:, 1][:, None, :]
    )
    hidden = (
        (jax.nn.silu(gate_act) * up_act * fast_hidden[:, 2][:, None, :])
        .astype(BF16)
        .reshape(all_rows, hidden_cols)
    )
    down_part = jnp.dot(hidden, w_down, preferred_element_type=F32).astype(BF16)
    half = width // 2
    mean_rows = call_linked(
        functools.partial(final_kernel, lines), 3,
        jax.ShapeDtypeStruct((2, batch_rows, half), BF16),
        [
            pltpu.VMEM((own_rows, half), F32),
            pltpu.VMEM((own_rows, half), BF16),
            pltpu.VMEM((own_rows, half), BF16),
            pltpu.VMEM((own_rows, half), F32),
            pltpu.VMEM((own_rows, half), F32),
            pltpu.VMEM((own_rows, half), BF16),
        ]
        + gather_scratch(2)
        + [DMA((3,)), DMA((3,))]
        + sum_scratch(lines, own_rows, width),
        (down_part, middle, own_scale, norm_gains[2:3]),
    )
    logits, stats = score(mean_rows, targets, lm_head)
    stats = stats[:, :8].T
    devices = 2 * tp_count
    mean_logits, logprob = call_linked(
        functools.partial(close_kernel, tp_count), 4,
        [
            jax.ShapeDtypeStruct((batch_rows, lm_head.shape[1]), BF16),
            jax.ShapeDtypeStruct((1, batch_rows), F32),
        ],
        [pltpu.VMEM((devices, 8, batch_rows), F32), DMA, DMA((devices,)), DMA((devices,))],
        (logits, stats),
    )
    return (mean_logits, logprob[0])


def body(*args):
    stream_in, lengths, fast_in = args[0], args[2], args[10]
    tp_count = lax.axis_size("tp")
    lines = tp_count // QUAD
    whole_tiles = stream_in.shape[0] % 16 == 0
    two_halves = lax.axis_size("member") == 2 and fast_in.shape[0] == 2
    even_lines = tp_count % QUAD == 0 and lines % 4 == 0
    pairs = stream_in.shape[0] * tp_count == 2 * lengths.shape[0] and lines == 4
    if whole_tiles and two_halves and even_lines and pairs:
        return linked_body(*args)
    return plain_body(*args)


def solution(mesh):
    in_specs = (
        P(("member", "tp"), None),
        P(("member", "tp"), None, None),
        P(),
        P(),
        P(),
        P(None, "tp"),
        P("tp", None),
        P(None, None, "tp"),
        P("tp", None),
        P(None, "tp"),
        P("member", None, None),
        P("member", None, "tp"),
        P("member", None),
    )
    out_specs = (P(None, "tp"), P())
    return jax.shard_map(body, mesh=mesh, in_specs=in_specs, out_specs=out_specs, check_vma=False)
```

```python
import functools

import jax
import jax.numpy as jnp
from jax import lax
from jax.experimental import pallas as pl
from jax.experimental.pallas import tpu as pltpu
from jax.sharding import PartitionSpec as P

HEADS = 32
KV = 8
HD = 128
CACHE = 512


ROPE_BASE = 500000.0


def rms_norm(values_in, gain):
    return (
        values_in
        * lax.rsqrt(jnp.mean(values_in * values_in, axis=-1, keepdims=True) + 1e-05)
        * gain
    )


def rotate(values_in, positions):
    half_dim = values_in.shape[-1] // 2
    frequency = ROPE_BASE ** (-jnp.arange(half_dim, dtype=jnp.float32) * 2.0 / values_in.shape[-1])
    angles = positions.astype(jnp.float32)[:, None, None] * frequency[None, None, :]
    lower_half = values_in[..., :half_dim]
    upper_half = values_in[..., half_dim:]
    return jnp.concatenate(
        [
            lower_half * jnp.cos(angles) - upper_half * jnp.sin(angles),
            upper_half * jnp.cos(angles) + lower_half * jnp.sin(angles),
        ],
        axis=-1,
    )


def attend(projected, cache_rows, positions):
    row_count = projected.shape[0]
    head_cols = HEADS * HD
    kv_cols = KV * HD
    queries = rotate(
        projected[:, :head_cols].astype(jnp.float32).reshape(row_count, HEADS, HD), positions
    ).astype(jnp.bfloat16)
    new_key = rotate(
        projected[:, head_cols : head_cols + kv_cols]
        .astype(jnp.float32)
        .reshape(row_count, KV, HD),
        positions,
    ).astype(jnp.bfloat16)
    new_value = projected[:, head_cols + kv_cols :].reshape(row_count, KV, HD)
    cache_keys = cache_rows[:, :, :kv_cols].reshape(row_count, CACHE, KV, HD)
    cache_values = cache_rows[:, :, kv_cols:].reshape(row_count, CACHE, KV, HD)
    grouped = queries.reshape(row_count, KV, HEADS // KV, HD)
    inv_root = HD ** (-0.5)
    cached = (
        jnp.einsum("rkgd,rckd->rkgc", grouped, cache_keys, preferred_element_type=jnp.float32)
        * inv_root
    )
    fresh = (
        jnp.einsum("rkgd,rkd->rkg", grouped, new_key, preferred_element_type=jnp.float32) * inv_root
    )
    in_cache = jnp.arange(CACHE)[None, :] < positions[:, None]
    cached = jnp.where(in_cache[:, None, None, :], cached, -1e30)
    peak = jnp.maximum(jnp.max(cached, axis=-1), fresh)
    weights = jnp.exp(cached - peak[..., None])
    fresh_w = jnp.exp(fresh - peak)
    total_sum = jnp.sum(weights, axis=-1) + fresh_w
    probs = (weights / total_sum[..., None]).astype(jnp.bfloat16)
    fresh_p = (fresh_w / total_sum).astype(jnp.bfloat16)
    result = jnp.einsum("rkgc,rckd->rkgd", probs, cache_values, preferred_element_type=jnp.float32)
    result = (
        result
        + fresh_p.astype(jnp.float32)[..., None] * new_value.astype(jnp.float32)[:, :, None, :]
    )
    return result.reshape(row_count, HEADS * HD).astype(jnp.bfloat16)


def plain_body(
    stream_in,
    kv_cache,
    lengths,
    targets,
    norm_gains,
    w_qkv,
    w_out,
    w_gate_up,
    w_down,
    lm_head,
    fast_in,
    fast_hidden,
    fast_out,
):
    tp_count = lax.axis_size("tp")
    tp_rank = lax.axis_index("tp")
    mem_dev = fast_in.shape[0]
    batch_rows = lengths.shape[0]
    own_rows = stream_in.shape[0]
    all_rows = own_rows * tp_count
    width = stream_in.shape[1]
    first_row = tp_rank * own_rows
    positions = lax.dynamic_slice_in_dim(lengths, first_row % batch_rows, own_rows, 0)
    own_member = first_row // batch_rows
    own_scale = lax.dynamic_index_in_dim(fast_out, own_member, 0, keepdims=True)
    own_normed = rms_norm(stream_in.astype(jnp.float32), norm_gains[0]).astype(jnp.bfloat16)
    attn_in = lax.all_gather(own_normed, "tp", axis=0, tiled=True)
    projected = jnp.dot(attn_in, w_qkv, preferred_element_type=jnp.float32).astype(jnp.bfloat16)
    row_major = lax.all_to_all(projected, "tp", split_axis=0, concat_axis=1, tiled=True)
    attended = attend(row_major, kv_cache, positions)
    head_major = lax.all_to_all(attended, "tp", split_axis=1, concat_axis=0, tiled=True)
    picked = head_major
    attn_sum = lax.psum_scatter(
        jnp.dot(picked, w_out, preferred_element_type=jnp.float32),
        "tp",
        scatter_dimension=0,
        tiled=True,
    )
    middle = (stream_in.astype(jnp.float32) + attn_sum).astype(jnp.bfloat16)
    own_ffn = rms_norm(middle.astype(jnp.float32), norm_gains[1]).astype(jnp.bfloat16)
    ffn_in = lax.all_gather(own_ffn, "tp", axis=0, tiled=True)
    grouped = ffn_in.astype(jnp.float32).reshape(mem_dev, batch_rows, width)
    gate_in = (grouped * fast_in[:, 0][:, None, :]).astype(jnp.bfloat16).reshape(all_rows, width)
    up_in = (grouped * fast_in[:, 1][:, None, :]).astype(jnp.bfloat16).reshape(all_rows, width)
    hidden_cols = w_gate_up.shape[2]
    gate_act = (
        jnp.dot(gate_in, w_gate_up[0], preferred_element_type=jnp.float32).reshape(
            mem_dev, batch_rows, hidden_cols
        )
        * fast_hidden[:, 0][:, None, :]
    )
    up_act = (
        jnp.dot(up_in, w_gate_up[1], preferred_element_type=jnp.float32).reshape(
            mem_dev, batch_rows, hidden_cols
        )
        * fast_hidden[:, 1][:, None, :]
    )
    hidden = (
        (jax.nn.silu(gate_act) * up_act * fast_hidden[:, 2][:, None, :])
        .astype(jnp.bfloat16)
        .reshape(all_rows, hidden_cols)
    )
    picked = hidden
    down_sum = lax.psum_scatter(
        jnp.dot(picked, w_down, preferred_element_type=jnp.float32),
        "tp",
        scatter_dimension=0,
        tiled=True,
    )
    layer_out = (middle.astype(jnp.float32) + down_sum * own_scale).astype(jnp.bfloat16)
    own_final = rms_norm(layer_out.astype(jnp.float32), norm_gains[2]).astype(jnp.bfloat16)
    final_in = lax.all_gather(own_final, "tp", axis=0, tiled=True)
    logits = jnp.dot(final_in, lm_head, preferred_element_type=jnp.float32)
    vocab_cols = lm_head.shape[1]
    member_total = jnp.sum(logits.reshape(mem_dev, batch_rows, vocab_cols), axis=0)
    member_count = mem_dev * lax.axis_size("member")
    mean_logit = (
        lax.psum(member_total.astype(jnp.bfloat16), "member").astype(jnp.float32) / member_count
    )
    column_ids = tp_rank * vocab_cols + jnp.arange(vocab_cols)
    target_part = jnp.sum(
        jnp.where(column_ids[None, :] == targets[:, None], mean_logit, 0.0), axis=-1
    )
    local_peak = jnp.max(mean_logit, axis=-1)
    peak = lax.pmax(local_peak, "tp")
    exp_total, target_logit = lax.psum(
        (jnp.sum(jnp.exp(mean_logit - peak[:, None]), axis=-1), target_part), "tp"
    )
    token_logprob = target_logit - (peak + jnp.log(exp_total))
    return (mean_logit.astype(jnp.bfloat16), token_logprob)


BF16 = jnp.bfloat16
F32 = jnp.float32
DMA = pltpu.SemaphoreType.DMA
QUAD = 4


def norm_rows(values_in, gain):
    return (
        values_in
        * lax.rsqrt(jnp.mean(values_in * values_in, axis=-1, keepdims=True) + 1e-05)
        * gain
    )


class Place:
    def __init__(self, lines):
        self.tp = lax.axis_index("tp")
        self.member = lax.axis_index("member")
        self.lines = lines
        self.quad = lax.rem(self.tp, QUAD)
        self.line = self.tp // QUAD
        self.quad_x = self.quad + 1 - 2 * lax.rem(self.quad, 2)
        self.quad_y = lax.rem(self.quad + 2, QUAD)
        self.quad_d = self.quad_x + self.quad_y - self.quad
        self.to_x = {"tp": self.line * QUAD + self.quad_x}
        self.to_y = {"tp": self.line * QUAD + self.quad_y}

    def line_at(self, step):
        return lax.rem(self.line + step + self.lines, self.lines)

    def to_line(self, step):
        return {"tp": self.line_at(step) * QUAD + self.quad}


def remote(src, dst, send_sem, recv_sem, device):
    copy = pltpu.make_async_remote_copy(
        src_ref=src,
        dst_ref=dst,
        send_sem=send_sem,
        recv_sem=recv_sem,
        device_id=device,
        device_id_type=pl.DeviceIdType.MESH,
    )
    copy.start()
    return copy


def greet(devices):
    barrier = pltpu.get_barrier_semaphore()
    for device in devices:
        pl.semaphore_signal(
            barrier, inc=1, device_id=device, device_id_type=pl.DeviceIdType.MESH
        )
    pl.semaphore_wait(barrier, len(devices))


def gather_rows(place, own, out, sems, line_steps, block_of):
    local_sem, sends, recvs = sems
    rows, cols = own.shape
    half = cols // 2

    def rows_of(step, quad):
        return pl.ds(pl.multiple_of(block_of(step, quad) * rows, rows), rows)

    mine = out.at[rows_of(0, place.quad)]
    local = pltpu.make_async_copy(own, mine, local_sem)
    local.start()
    line_copies = []
    for k, step in enumerate(line_steps):
        if k:
            line_copies.append(
                remote(own, mine, sends.at[0, k], recvs.at[0, k], place.to_line(step))
            )
        else:
            line_copies.append(None)
    by_x, by_y, over_x, over_y = [], [], [], []

    def spread(k):
        block = own if k == 0 else out.at[rows_of(-line_steps[k], place.quad)]
        into = out.at[rows_of(-line_steps[k], place.quad)]
        by_x.append(remote(block, into, sends.at[1, k], recvs.at[1, k], place.to_x))
        by_y.append(remote(block, into, sends.at[2, k], recvs.at[2, k], place.to_y))

    def relay(k):
        by_x[k].wait_recv()
        from_x = out.at[rows_of(-line_steps[k], place.quad_x), pl.ds(0, half)]
        over_y.append(remote(from_x, from_x, sends.at[3, k], recvs.at[3, k], place.to_y))
        by_y[k].wait_recv()
        from_y = out.at[rows_of(-line_steps[k], place.quad_y), pl.ds(half, half)]
        over_x.append(remote(from_y, from_y, sends.at[4, k], recvs.at[4, k], place.to_x))

    spread(0)
    for k in range(1, len(line_steps)):
        line_copies[k].wait_recv()
        spread(k)
        relay(k - 1)
    relay(len(line_steps) - 1)
    for k in range(len(line_steps)):
        over_y[k].wait_recv()
        over_x[k].wait_recv()
    local.wait()
    for copies in (line_copies, by_x, by_y, over_x, over_y):
        for copy in copies:
            if copy is not None:
                copy.wait_send()


def sum_rows(place, part, sems, bufs):
    sends, recvs = sems
    got_dx, got_dy, put_x, put_y, got_x, got_y, put_z, got_z = bufs
    rows = got_x.shape[1]
    half = got_dx.shape[2]
    low, high = pl.ds(0, half), pl.ds(half, half)
    steps = list(range(1, place.lines)) + [0]

    def rows_of(step, quad):
        index = place.line_at(step) * QUAD + quad
        return pl.ds(pl.multiple_of(index * rows, rows), rows)

    d_x, d_y, x_high, y_low, x_low, y_high, z_copies = {}, {}, {}, {}, {}, {}, {}
    for k in steps:
        diag = rows_of(k, place.quad_d)
        d_x[k] = remote(part.at[diag, high], got_dx.at[k], sends.at[0, k], recvs.at[0, k], place.to_x)
        d_y[k] = remote(part.at[diag, low], got_dy.at[k], sends.at[1, k], recvs.at[1, k], place.to_y)
    for k in steps:
        x_high[k] = remote(
            part.at[rows_of(k, place.quad_x), high], got_x.at[k, :, high],
            sends.at[2, k], recvs.at[2, k], place.to_x,
        )
        y_low[k] = remote(
            part.at[rows_of(k, place.quad_y), low], got_y.at[k, :, low],
            sends.at[3, k], recvs.at[3, k], place.to_y,
        )
        d_y[k].wait_recv()
        put_x[k] = (
            part[rows_of(k, place.quad_x), low].astype(F32) + got_dy[k].astype(F32)
        ).astype(BF16)
        x_low[k] = remote(
            put_x.at[k], got_x.at[k, :, low], sends.at[4, k], recvs.at[4, k], place.to_x
        )
        d_x[k].wait_recv()
        put_y[k] = (
            part[rows_of(k, place.quad_y), high].astype(F32) + got_dx[k].astype(F32)
        ).astype(BF16)
        y_high[k] = remote(
            put_y.at[k], got_y.at[k, :, high], sends.at[5, k], recvs.at[5, k], place.to_y
        )
    total = None
    for k in steps:
        for copies in (x_high, y_low, x_low, y_high):
            copies[k].wait_recv()
        quad_sum = (
            part[rows_of(k, place.quad), :].astype(F32)
            + got_x[k].astype(F32)
            + got_y[k].astype(F32)
        )
        if k:
            put_z[k] = quad_sum.astype(BF16)
            z_copies[k] = remote(
                put_z.at[k], got_z.at[k], sends.at[6, k], recvs.at[6, k], place.to_line(k)
            )
        else:
            total = quad_sum
    for k in steps[:-1]:
        z_copies[k].wait_recv()
        total = total + got_z[k].astype(F32)
    for copies in (d_x, d_y, x_high, y_low, x_low, y_high, z_copies):
        for copy in copies.values():
            copy.wait_send()
    return total


def near(place):
    return [place.to_x, place.to_y] + [place.to_line(k) for k in range(1, place.lines)]


def gather_kernel(lines, stream, gain, out, own, local_sem, sends, recvs):
    place = Place(lines)
    own[...] = norm_rows(stream[...].astype(F32), gain[...]).astype(BF16)
    greet(near(place))
    gather_rows(
        place, own, out, (local_sem, sends, recvs), list(range(lines)),
        lambda step, quad: place.line_at(step) * QUAD + quad,
    )


def tail_kernel(
    lines, heads_in, w_out, stream, gains, fast_in, fast_hidden, scale, targets, w_gate_up, w_down, lm_head,
    out, logprob,
    part, middle, ffn_in, acts, hidden, gate_up, down, words, own, half_own, away, from_core,
    pair, from_pair, mean, rows_in, stats, table,
    load_sems, tile_sends, tile_recvs, stat_sends, stat_recvs, side_sends, side_recvs,
    local_sem, sends, recvs, last_sem, last_sends, last_recvs, *sums
):
    place = Place(lines)
    tp_count = lines * QUAD
    member = place.member
    cols = words.shape[1]
    other = {"member": 1 - member}
    loads = [
        pltpu.make_async_copy(w_gate_up, gate_up, load_sems.at[0]),
        pltpu.make_async_copy(w_down, down, load_sems.at[1]),
        pltpu.make_async_copy(
            lm_head.at[:, pl.ds(pl.multiple_of(member * cols, cols), cols)], words, load_sems.at[2]
        ),
    ]
    for load in loads:
        load.start()
    others = []
    for core in (member, 1 - member):
        for step in range(tp_count):
            if others or step:
                others.append({"member": core, "tp": lax.rem(place.tp + step, tp_count)})
    greet(others)
    wide = 512

    @pl.loop(0, part.shape[1] // wide)
    def _(i):
        span = pl.ds(pl.multiple_of(i * wide, wide), wide)
        part[:, span] = jnp.dot(
            heads_in[...], w_out[:, span], preferred_element_type=F32
        ).astype(BF16)

    count = len(sums) // 2
    total = sum_rows(place, part, sums[:2], sums[2:count])
    middle[...] = (stream[...].astype(F32) + total).astype(BF16)
    own[...] = norm_rows(middle[...].astype(F32), gains[1][:1]).astype(BF16)
    gather_rows(
        place, own, ffn_in, (local_sem, sends, recvs), list(range(lines)),
        lambda step, quad: place.line_at(step) * QUAD + quad,
    )
    loads[0].wait()
    members = fast_in.shape[0]
    batch_rows = ffn_in.shape[0] // members
    acts[...] = jnp.zeros_like(acts)

    @pl.loop(0, ffn_in.shape[1] // wide)
    def _(i):
        span = pl.ds(pl.multiple_of(i * wide, wide), wide)
        values = ffn_in[:, span].astype(F32)
        for j in range(2):
            scaled = jnp.concatenate(
                [
                    values[m * batch_rows : (m + 1) * batch_rows] * fast_in[m, j, :, span][:1]
                    for m in range(members)
                ],
                axis=0,
            ).astype(BF16)
            acts[j] += jnp.dot(scaled, gate_up[j, span, :], preferred_element_type=F32)

    for m in range(members):
        rows = slice(m * batch_rows, (m + 1) * batch_rows)
        gate = acts[0, rows, :] * fast_hidden[m, 0][:1]
        hidden[rows, :] = (
            gate / (1.0 + jnp.exp(-gate))
            * (acts[1, rows, :] * fast_hidden[m, 1][:1])
            * fast_hidden[m, 2][:1]
        ).astype(BF16)
    loads[1].wait()

    @pl.loop(0, part.shape[1] // wide)
    def _(i):
        span = pl.ds(pl.multiple_of(i * wide, wide), wide)
        part[:, span] = jnp.dot(
            hidden[...], down[:, span], preferred_element_type=F32
        ).astype(BF16)

    total = sum_rows(place, part, sums[count : count + 2], sums[count + 2 :])
    layer_out = (middle[...].astype(F32) + total * scale[...]).astype(BF16)
    normed = norm_rows(layer_out.astype(F32), gains[2][:1]).astype(BF16)
    half = mean.shape[1]
    first = member == 0
    low, high = normed[:, :half].astype(F32), normed[:, half:].astype(F32)
    half_own[...] = jnp.where(first, low, high)
    away[...] = jnp.where(first, high, low).astype(BF16)
    core = remote(away, from_core, side_sends.at[0], side_recvs.at[0], other)
    core.wait_recv()
    half_own[...] = half_own[...] + from_core[...].astype(F32)
    pair[...] = half_own[...]
    twin = remote(
        pair, from_pair, side_sends.at[1], side_recvs.at[1], place.to_line(lines // 2)
    )
    twin.wait_recv()
    mean[...] = ((half_own[...] + from_pair[...]) * 0.25).astype(BF16)
    turn = 1 - 2 * lax.rem(place.line, 2)

    class Pairwise:
        pass

    near_line = Pairwise()
    near_line.quad, near_line.quad_x, near_line.quad_y = place.quad, place.quad_x, place.quad_y
    near_line.to_x, near_line.to_y = place.to_x, place.to_y
    near_line.to_line = lambda step: {"tp": (place.line + turn) * QUAD + place.quad}
    mine = rows_in.at[member]
    gather_rows(
        near_line, mean, mine, (last_sem, last_sends, last_recvs), [0, 1],
        lambda step, quad: lax.rem(place.line + abs(step), 2) * QUAD + quad,
    )
    share = remote(mine, mine, side_sends.at[2], side_recvs.at[2], other)
    loads[2].wait()
    share.wait_recv()
    tile_width = cols // tile_sends.shape[0]
    batch = rows_in.shape[1]
    peak = jnp.full((batch, 1), -jnp.inf, F32)
    amount = jnp.zeros((batch, 1), F32)
    found = jnp.zeros((batch, 1), F32)
    tiles = []
    for i in range(tile_sends.shape[0]):
        span = pl.ds(i * tile_width, tile_width)
        tile = jnp.dot(rows_in[0], words[:half, span], preferred_element_type=F32) + jnp.dot(
            rows_in[1], words[half:, span], preferred_element_type=F32
        )
        into = out.at[:, pl.ds(pl.multiple_of(member * cols + i * tile_width, tile_width), tile_width)]
        into[...] = tile.astype(BF16)
        tiles.append(remote(into, into, tile_sends.at[i], tile_recvs.at[i], other))
        new = jnp.maximum(peak, jnp.max(tile, axis=-1, keepdims=True))
        amount = amount * jnp.exp(peak - new) + jnp.sum(
            jnp.exp(tile - new), axis=-1, keepdims=True
        )
        peak = new
        column = (
            (place.tp * 2 + member) * cols
            + i * tile_width
            + lax.broadcasted_iota(jnp.int32, tile.shape, 1)
        )
        found = found + jnp.sum(
            jnp.where(column == targets[...], tile, 0.0), axis=-1, keepdims=True
        )
    lane = lax.broadcasted_iota(jnp.int32, (batch, 128), 1)
    block = jnp.where(lane == 0, peak, jnp.where(lane == 1, amount, found))
    stats[...] = jnp.transpose(block)[:8, :]
    copies = []
    for slot, device in enumerate(others):
        copies.append(
            remote(stats, table.at[slot + 1], stat_sends.at[slot], stat_recvs.at[slot], device)
        )
    table[0] = stats[...]
    for copy in copies:
        copy.wait_recv()
    top = jnp.max(table[:, 0, :], axis=0, keepdims=True)
    amount = jnp.sum(table[:, 1, :] * jnp.exp(table[:, 0, :] - top), axis=0, keepdims=True)
    found = jnp.sum(table[:, 2, :], axis=0, keepdims=True)
    logprob[...] = found - (top + jnp.log(amount))
    for copy in tiles:
        copy.wait_recv()
    for copy in [core, twin, share] + tiles + copies:
        copy.wait_send()


VMEM = pl.BlockSpec(memory_space=pltpu.VMEM)
ANY = pl.BlockSpec(memory_space=pl.ANY)
MIB = 1024 * 1024


def call_linked(kernel, number, out_shape, scratch, args, mib, far=0):
    return pl.pallas_call(
        kernel,
        out_shape=out_shape,
        in_specs=[VMEM] * (len(args) - far) + [ANY] * far,
        out_specs=jax.tree.map(lambda _: VMEM, out_shape),
        scratch_shapes=scratch,
        compiler_params=pltpu.CompilerParams(
            collective_id=number, has_side_effects=True, vmem_limit_bytes=mib * MIB
        ),
        cost_estimate=pl.CostEstimate(flops=0, bytes_accessed=64 * MIB, transcendentals=0),
    )(*args)


def gather_scratch(lines):
    return [DMA, DMA((5, lines)), DMA((5, lines))]


def sum_scratch(lines, rows, cols):
    small = pltpu.VMEM((lines, rows, cols // 2), BF16)
    large = pltpu.VMEM((lines, rows, cols), BF16)
    return [DMA((7, lines)), DMA((7, lines)), small, small, small, small, large, large, large, large]


def attend_kernel(positions, query, fresh_key, fresh_value, cache, out):
    row = pl.program_id(0)
    heads, head_size = query.shape[1], query.shape[2]
    kv_cols = cache.shape[2] // 2
    key_heads = kv_cols // head_size
    group = heads // key_heads
    count = cache.shape[1]
    query_row = query[0].astype(F32)
    inv_root = head_size ** (-0.5)
    wide = jnp.concatenate([query_row] * key_heads, axis=1)
    owner = lax.broadcasted_iota(jnp.int32, wide.shape, 0) // group
    column = lax.broadcasted_iota(jnp.int32, wide.shape, 1) // head_size
    wide = jnp.where(owner == column, wide, 0.0).astype(BF16)
    scores = (
        lax.dot_general(
            wide, cache[0, :, :kv_cols], (((1,), (1,)), ((), ())), preferred_element_type=F32
        )
        * inv_root
    )
    spot = lax.broadcasted_iota(jnp.int32, scores.shape, 1)
    scores = jnp.where(spot < positions[row], scores, -1e30)
    fresh = jnp.sum(query_row * fresh_key[0].astype(F32), axis=-1, keepdims=True) * inv_root
    peak = jnp.maximum(jnp.max(scores, axis=-1, keepdims=True), fresh)
    weights = jnp.exp(scores - peak)
    fresh_w = jnp.exp(fresh - peak)
    total_sum = jnp.sum(weights, axis=-1, keepdims=True) + fresh_w
    probs = (weights / total_sum).astype(BF16)
    fresh_p = (fresh_w / total_sum).astype(BF16).astype(F32)
    full = jnp.dot(probs, cache[0, :, kv_cols:], preferred_element_type=F32)
    full = jnp.where(owner == column, full, 0.0)
    result = full[:, :head_size]
    for k in range(1, key_heads):
        result = result + full[:, k * head_size : (k + 1) * head_size]
    out[0] = (result + fresh_p * fresh_value[0].astype(F32)).astype(BF16)


def attend_rows(projected, cache_rows, positions):
    rows = projected.shape[0]
    head_cols, kv_cols = HEADS * HD, KV * HD
    group = HEADS // KV
    queries = rotate(
        projected[:, :head_cols].astype(F32).reshape(rows, HEADS, HD), positions
    ).astype(BF16)
    new_key = rotate(
        projected[:, head_cols : head_cols + kv_cols].astype(F32).reshape(rows, KV, HD), positions
    ).astype(BF16)
    new_value = projected[:, head_cols + kv_cols :].reshape(rows, KV, HD)
    new_key = jnp.repeat(new_key, group, axis=1)
    new_value = jnp.repeat(new_value, group, axis=1)
    per_row = pl.BlockSpec((1, HEADS, HD), lambda r, p: (r, 0, 0))
    cache_spec = pl.BlockSpec((1,) + cache_rows.shape[1:], lambda r, p: (r, 0, 0))
    result = pl.pallas_call(
        attend_kernel,
        grid_spec=pltpu.PrefetchScalarGridSpec(
            num_scalar_prefetch=1,
            grid=(rows,),
            in_specs=[per_row, per_row, per_row, cache_spec],
            out_specs=per_row,
        ),
        out_shape=jax.ShapeDtypeStruct((rows, HEADS, HD), BF16),
        compiler_params=pltpu.CompilerParams(vmem_limit_bytes=32 * 1024 * 1024),
    )(positions, queries, new_key, new_value, cache_rows)
    return result.reshape(rows, head_cols)


def whole_tiles(rows):
    return jnp.broadcast_to(rows[..., None, :], rows.shape[:-1] + (8, rows.shape[-1]))


def linked_body(
    stream_in,
    kv_cache,
    lengths,
    targets,
    norm_gains,
    w_qkv,
    w_out,
    w_gate_up,
    w_down,
    lm_head,
    fast_in,
    fast_hidden,
    fast_out,
):
    tp_count = lax.axis_size("tp")
    tp_rank = lax.axis_index("tp")
    lines = tp_count // QUAD
    batch_rows = lengths.shape[0]
    own_rows, width = stream_in.shape
    all_rows = own_rows * tp_count
    first_row = tp_rank * own_rows
    positions = lax.dynamic_slice_in_dim(lengths, first_row % batch_rows, own_rows, 0)
    own_member = first_row // batch_rows
    own_scale = lax.dynamic_index_in_dim(fast_out, own_member, 0, keepdims=True)
    all_shape = jax.ShapeDtypeStruct((all_rows, width), BF16)
    own_buf = pltpu.VMEM((own_rows, width), BF16)

    attn_in = call_linked(
        functools.partial(gather_kernel, lines), 1, all_shape,
        [own_buf] + gather_scratch(lines), (stream_in, norm_gains[0:1]), 16,
    )
    projected = jnp.dot(attn_in, w_qkv, preferred_element_type=F32).astype(BF16)
    row_major = lax.all_to_all(projected, "tp", split_axis=0, concat_axis=1, tiled=True)
    attended = attend_rows(row_major, kv_cache, positions)
    head_major = lax.all_to_all(attended, "tp", split_axis=1, concat_axis=0, tiled=True)
    half = width // 2
    devices = 2 * tp_count
    vocab_cols = lm_head.shape[1]
    tiles = 4
    mean_logits, logprob = call_linked(
        functools.partial(tail_kernel, lines), 2,
        [
            jax.ShapeDtypeStruct((batch_rows, vocab_cols), BF16),
            jax.ShapeDtypeStruct((1, batch_rows), F32),
        ],
        [
            pltpu.VMEM((all_rows, width), BF16),
            own_buf,
            pltpu.VMEM((all_rows, width), BF16),
            pltpu.VMEM((2, all_rows, w_gate_up.shape[2]), F32),
            pltpu.VMEM((all_rows, w_gate_up.shape[2]), BF16),
            pltpu.VMEM(w_gate_up.shape, BF16),
            pltpu.VMEM(w_down.shape, BF16),
            pltpu.VMEM((width, vocab_cols // 2), BF16),
            own_buf,
            pltpu.VMEM((own_rows, half), F32),
            pltpu.VMEM((own_rows, half), BF16),
            pltpu.VMEM((own_rows, half), BF16),
            pltpu.VMEM((own_rows, half), F32),
            pltpu.VMEM((own_rows, half), F32),
            pltpu.VMEM((own_rows, half), BF16),
            pltpu.VMEM((2, batch_rows, half), BF16),
            pltpu.VMEM((8, batch_rows), F32),
            pltpu.VMEM((devices, 8, batch_rows), F32),
            DMA((3,)), DMA((tiles,)), DMA((tiles,)), DMA((devices,)), DMA((devices,)), DMA((3,)), DMA((3,)),
        ]
        + gather_scratch(lines)
        + gather_scratch(2)
        + sum_scratch(lines, own_rows, width)
        + sum_scratch(lines, own_rows, width),
        (
            head_major, w_out, stream_in, whole_tiles(norm_gains), whole_tiles(fast_in),
            whole_tiles(fast_hidden), own_scale, targets[:, None],
            w_gate_up, w_down, lm_head,
        ),
        58, 3,
    )
    return (mean_logits, logprob[0])


def body(*args):
    stream_in, lengths, fast_in = args[0], args[2], args[10]
    tp_count = lax.axis_size("tp")
    lines = tp_count // QUAD
    full_rows = stream_in.shape[0] % 16 == 0
    two_halves = lax.axis_size("member") == 2 and fast_in.shape[0] == 2
    even_lines = tp_count % QUAD == 0 and lines % 4 == 0
    pairs = stream_in.shape[0] * tp_count == 2 * lengths.shape[0] and lines == 4
    if full_rows and two_halves and even_lines and pairs:
        return linked_body(*args)
    return plain_body(*args)


def solution(mesh):
    in_specs = (
        P(("member", "tp"), None),
        P(("member", "tp"), None, None),
        P(),
        P(),
        P(),
        P(None, "tp"),
        P("tp", None),
        P(None, None, "tp"),
        P("tp", None),
        P(None, "tp"),
        P("member", None, None),
        P("member", None, "tp"),
        P("member", None),
    )
    out_specs = (P(None, "tp"), P())
    return jax.shard_map(body, mesh=mesh, in_specs=in_specs, out_specs=out_specs, check_vma=False)
```
